32 devices in a mesh: scen: 2 (over y), col: 16 (over z, x, core).
Axes of the slice: x: 2, y: 2, z: 4, core: 2. Of those that a mesh axis runs over, the one named last changes fastest.
Arguments:
- border: float32 [4, 1536, 16384], P('scen', None, 'col'), may hold values from -6 to 6
- barrier: float32 [4, 1536], P('scen'), may hold values from 0.1 to 10
- row_counts: int32 [4], P('scen'), may hold values from 1024 to 1536, as said below
Outputs:
- factor_panel: float32 [16, 2, 512, 512], P('col', 'scen')
The draws below stay inside these ranges and needn't reach their ends.
Inputs may be any that keep to these rules, and one draw needn't show every extreme that they name: `row_counts`: every value lies between 1024 and 1536, and at least one scenario uses all 1536 rows.
All inputs are finite; a program needn't handle non-finite values.
Results may differ from the reference program's by a relative error of at most 0.0003.
Values sent between devices are 32-bit elements; how exact they have to be, the bound alone decides.
A program may use at most 64 MiB of HBM per device.

```python
import math
import jax
import jax.numpy as jnp
from jax import lax

NB = 16384
PANEL = 512
RMAX = 1536
SCEN = 4
N_SCEN = 2
N_COL = 16


def draw_row_counts(key, part):
    counts = jax.random.randint(jax.random.fold_in(key, 11), (SCEN,), 2 * RMAX // 3, RMAX + 1)
    chosen = jax.random.randint(jax.random.fold_in(key, 23), (), 0, SCEN)
    return jnp.where(jnp.arange(SCEN) == chosen, RMAX, counts).astype(jnp.int32)


def block_levels(key, dims, cuts, smallest, high):
    gain = 1.0
    for position, parts in cuts:
        steps = jax.random.uniform(jax.random.fold_in(jax.random.fold_in(key, 6), position), (parts,), jnp.float32, smallest / len(cuts), high / len(cuts))
        gain = gain * jnp.repeat(jnp.exp(steps), dims[position] // parts).reshape((-1,) + (1,) * (len(dims) - 1 - position))
    return gain


def gaussian(key, extent, scale, reach, pieces=(), held_as=jnp.bfloat16):
    result = jax.random.normal(key, extent, jnp.float32) * scale
    if len(pieces) > 0:
        result = block_levels(key, extent, pieces, -0.22, 0.18) * result
    return jnp.clip(result, min=-reach, max=reach).astype(held_as)


def setup_inputs(seed: int = 0) -> dict:
    key_of = jax.random.split(jax.random.key(seed), 4)
    return {
        "border": gaussian(key_of[0], (SCEN, RMAX, NB), 1.0, 6.0, ((0, 2), (2, 16)), jnp.float32),
        "barrier": jnp.clip(jnp.exp(math.log(10.0) - 4.6051702 * jax.random.uniform(key_of[1], (SCEN, RMAX), jnp.float32) ** block_levels(key_of[1], (SCEN, RMAX), ((0, 2),), -0.2, 0.2)), 0.1, 10.0),
        "row_counts": draw_row_counts(jax.random.fold_in(key_of[3], 71), 0),
    }


def reference(border, barrier, row_counts):
    positions = lax.iota(jnp.int32, RMAX)
    weights = jnp.where(positions[None, :] < row_counts[:, None], 1.0 / barrier, jnp.float32(0.0))
    split_cols = border.reshape(SCEN, RMAX, N_COL, NB // N_COL)
    panel_border = split_cols[:, :, :, :PANEL // N_COL].reshape(SCEN, RMAX, PANEL)

    def accumulate(carry, items):
        border_one, weight_one, panel_one = items
        weighted = border_one * weight_one[:, None]
        term = jnp.einsum('rc,rk->ck', weighted.astype(jnp.float32), panel_one.astype(jnp.float32), precision=lax.Precision.HIGHEST, preferred_element_type=jnp.float32)
        return (carry + term, None)
    schur, _ = lax.scan(accumulate, jnp.zeros((NB, PANEL), jnp.float32), (border, weights, panel_border))
    block = schur.reshape(N_COL, NB // N_COL, PANEL)[:, :PANEL // N_COL, :].reshape(PANEL, PANEL)
    lower = jnp.linalg.cholesky(block)
    solved = lax.linalg.triangular_solve(lower, schur, left_side=False, lower=True, transpose_a=True)
    return solved.reshape(N_COL, N_SCEN, NB // (N_COL * N_SCEN), PANEL)
```

```python
import jax
import jax.numpy as jnp
from jax import lax
from jax.experimental import pallas as pl
from jax.experimental.pallas import tpu as pltpu
from jax.sharding import PartitionSpec as P

PANEL = 512
TILE = 128
SUB = 8
TILES = PANEL // TILE
UPPER = [(j, k) for j in range(TILES) for k in range(j, TILES)]


def inverse_factor(a):
    lane = lax.broadcasted_iota(jnp.int32, (SUB, TILE), 1)
    sub = lax.broadcasted_iota(jnp.int32, (SUB, TILE), 0)
    rows = [a[SUB * t : SUB * (t + 1)] for t in range(TILE // SUB)]
    out = [jnp.zeros((SUB, TILE), jnp.float32) for _ in rows]
    for k in range(TILE):
        own, r = divmod(k, SUB)
        row = jnp.broadcast_to(rows[own][r : r + 1], (SUB, TILE))
        pivot = jnp.broadcast_to(rows[own][r : r + 1, k : k + 1], (SUB, TILE))
        done = jnp.where(lane < k, row, jnp.where(lane == k, 1.0, 0.0)) * lax.rsqrt(pivot)
        out[own] = jnp.where(sub == r, done, out[own])
        step = jnp.where(lane == k, 1.0, row) / pivot
        for t in range(own if r < SUB - 1 else own + 1, TILE // SUB):
            col = jnp.broadcast_to(rows[t][:, k : k + 1], (SUB, TILE))
            rows[t] = jnp.where(lane == k, 0.0, rows[t]) - col * step
    return jnp.concatenate(out, axis=0)


def factor_kernel(a_ref, b_ref, inv_ref, t_ref):
    t_ref[...] = jnp.zeros_like(t_ref)
    for n, (j, k) in enumerate(UPPER):
        t_ref[j * TILE : (j + 1) * TILE, k * TILE : (k + 1) * TILE] = a_ref[n] + b_ref[n]
    eye = (
        lax.broadcasted_iota(jnp.int32, (TILE, TILE), 0)
        == lax.broadcasted_iota(jnp.int32, (TILE, TILE), 1)
    ).astype(jnp.float32)
    for j in range(TILES):
        t_ref[j * TILE : (j + 1) * TILE, PANEL + j * TILE : PANEL + (j + 1) * TILE] = eye

    @pl.loop(0, TILES)
    def _(j):
        here = pl.ds(pl.multiple_of(j * TILE, TILE), TILE)
        inv = inverse_factor(t_ref[here, here])
        scaled = jnp.dot(
            inv, t_ref[here, :], precision=lax.Precision.HIGHEST, preferred_element_type=jnp.float32
        )
        inv_ref[here, :] = scaled[:, PANEL:]
        lane = lax.broadcasted_iota(jnp.int32, (TILE, PANEL), 1)
        ahead = jnp.where(lane >= (j + 1) * TILE, scaled[:, :PANEL], 0.0).T
        for i in range(1, TILES):

            @pl.when(i > j)
            def _():
                part = slice(i * TILE, (i + 1) * TILE)
                t_ref[part, :] -= jnp.dot(
                    ahead[part],
                    scaled,
                    precision=lax.Precision.HIGHEST,
                    preferred_element_type=jnp.float32,
                )


def inverse_of_factor(mine, other):
    return pl.pallas_call(
        factor_kernel,
        out_shape=jax.ShapeDtypeStruct((PANEL, PANEL), jnp.float32),
        in_specs=[pl.BlockSpec(memory_space=pltpu.VMEM)] * 2,
        out_specs=pl.BlockSpec(memory_space=pltpu.VMEM),
        scratch_shapes=[pltpu.VMEM((PANEL, 2 * PANEL), jnp.float32)],
        cost_estimate=pl.CostEstimate(
            flops=2 * 10**10, bytes_accessed=3 * 10**6, transcendentals=PANEL
        ),
        name="factor",
    )(mine, other)


def body(border, barrier, row_counts):
    scen_here, capacity, own_cols = border.shape
    n_scen = lax.axis_size("scen")
    per_owner = PANEL // lax.axis_size("col")
    rows_owned = own_cols // n_scen
    depth = scen_here * capacity
    positions = lax.iota(jnp.int32, capacity)
    weights = jnp.where(positions[None, :] < row_counts[:, None], 1.0 / barrier, jnp.float32(0.0))
    panel_part = jnp.transpose(border[:, :, :per_owner], (2, 0, 1)).reshape(per_owner, depth)
    panel = lax.all_gather(panel_part, "col", axis=0, tiled=True)
    weighted = panel * weights.reshape(1, depth)
    block = jnp.einsum(
        "pr,qr->pq", weighted, panel, precision=lax.Precision.HIGH,
        preferred_element_type=jnp.float32,
    )
    upper = jnp.stack(
        [block[j * TILE : (j + 1) * TILE, k * TILE : (k + 1) * TILE] for j, k in UPPER]
    )
    if n_scen == 2:
        swap = [(0, 1), (1, 0)]
        upper_other = lax.ppermute(upper, "scen", swap)
    else:
        upper_other = lax.psum(upper, "scen") - upper
    part = jnp.einsum(
        "pr,rc->pc", weighted, border.reshape(depth, own_cols), precision=lax.Precision.HIGH,
        preferred_element_type=jnp.float32,
    )
    if n_scen == 2:
        me = lax.axis_index("scen")
        sent = lax.dynamic_slice_in_dim(part, (1 - me) * rows_owned, rows_owned, 1)
        kept = lax.dynamic_slice_in_dim(part, me * rows_owned, rows_owned, 1)
        owned = kept + lax.ppermute(sent, "scen", swap)
    else:
        owned = lax.psum_scatter(part, "scen", scatter_dimension=1, tiled=True)
    inverse = inverse_of_factor(upper, upper_other)
    solved = jnp.einsum(
        "qt,pq->tp", owned, inverse, precision=lax.Precision.HIGHEST,
        preferred_element_type=jnp.float32,
    )
    return solved.reshape(1, 1, rows_owned, PANEL)


def solution(mesh):
    placed = (P("scen", None, "col"), P("scen", None), P("scen"))
    return jax.shard_map(
        body, mesh=mesh, in_specs=placed, out_specs=P("col", "scen", None, None), check_vma=False
    )
```
